128 devices in a mesh: dp: 8 (over x, core), rollout: 16 (over y, z).
Axes of the slice: x: 4, y: 4, z: 4, core: 2. Of those that a mesh axis runs over, the one named last changes fastest.
Arguments:
- queries: bfloat16 [128, 512, 2560], P(('dp', 'rollout')), may hold values from -100 to 100
- resp_keys: bfloat16 [128, 512, 512], P(('dp', 'rollout')), may hold values from -5 to 5
- resp_values: bfloat16 [128, 512, 512], P(('dp', 'rollout')), may hold values from -6 to 6
- prompt_keys: bfloat16 [8, 256, 512], P('dp', 'rollout'), may hold values from -6 to 6
- prompt_values: bfloat16 [8, 256, 512], P('dp', 'rollout'), may hold values from -6 to 6
- d_out: bfloat16 [128, 512, 2560], P(('dp', 'rollout')), may hold values from -6 to 6
- lengths: int32 [128], replicated, may hold values from 64 to 512
- owner: int32 [128], replicated, may hold values from 0 to 7
Outputs:
- attn_out: bfloat16 [128, 512, 2560], P(('dp', 'rollout'))
- d_queries: bfloat16 [128, 512, 2560], P(('dp', 'rollout'))
- d_resp_keys: bfloat16 [128, 512, 512], P(('dp', 'rollout'))
- d_resp_values: bfloat16 [128, 512, 512], P(('dp', 'rollout'))
- d_prompt_keys: float32 [8, 256, 512], P('dp', 'rollout')
- d_prompt_values: float32 [8, 256, 512], P('dp', 'rollout')
The draws below stay inside these ranges and needn't reach their ends.
Inputs may be any that keep to these rules, and one draw needn't show every extreme that they name: `lengths`: rows of a block at or past its length are padding.
All inputs are finite; a program needn't handle non-finite values.
Results may differ from the reference program's by a relative error of at most 0.0071.
Values may be sent and summed in bfloat16 or wider, within the bound.
No kernel may reach another device: no remote copies, remote signals or barrier semaphores. Data moves between devices by JAX's collectives and lax.ppermute only.
A program may use at most 128 MiB of HBM per device.

```python
import jax
import jax.numpy as jnp
from jax import lax

HEAD_DIM = 128
BLOCK = 512
TILE = 128
QW = 2560
KW = 512
PROMPT = 256
NB = 128
N_DP = 8


def twin_keys(key):
    base = jax.random.normal(jax.random.fold_in(key, 11), (NB, BLOCK, KW), jnp.float32)
    base = jnp.clip(base, -4.0, 4.0)
    return base


def draw_resp_keys(key, part):
    return twin_keys(key).astype(jnp.bfloat16)


def draw_queries(key, part):
    base = jnp.clip(jax.random.normal(jax.random.fold_in(key, 23), (NB, BLOCK, QW), jnp.float32), -6.0, 6.0)
    return base.astype(jnp.bfloat16)


def touch_ends(entries, rng, least, top_value):
    place = [jax.random.randint(jax.random.fold_in(rng, axis), (), 0, length) for axis, length in enumerate(entries.shape)]
    longest = entries.shape.index(max(entries.shape))
    next_to = place[:longest] + [(place[longest] + 1) % entries.shape[longest]] + place[longest + 1:]
    return entries.at[tuple(place)].set(least).at[tuple(next_to)].set(top_value)


def levels(own_key, shape, shards, low, high):
    def one(position, parts):
        draws = jax.random.uniform(jax.random.fold_in(jax.random.fold_in(own_key, 6), position), (parts,), jnp.float32, low / len(shards), high / len(shards))
        return jnp.repeat(jnp.exp(draws), shape[position] // parts).reshape((-1,) + (1,) * (len(shape) - position - 1))

    level = one(*shards[0])
    for cut in shards[1:]:
        level = level * one(*cut)
    return level


def scatter_about(own_key, shape, width, most, split=(), kind=jnp.bfloat16):
    array = jax.random.normal(own_key, shape, jnp.float32) * width
    if len(split) > 0:
        array = levels(own_key, shape, split, -0.22, 0.18) * array
    return jnp.clip(array, min=-most, max=most).astype(kind)


def setup_inputs(seed: int = 0) -> dict:
    splits = jax.random.split(jax.random.key(seed), 9)
    queries = draw_queries(jax.random.fold_in(splits[8], 71), 0)
    resp_keys = draw_resp_keys(jax.random.fold_in(splits[8], 71), 0)
    resp_values = scatter_about(splits[2], (NB, BLOCK, KW), 1.0, 6.0, ((0, 128),))
    prompt_keys = scatter_about(splits[3], (N_DP, PROMPT, KW), 1.0, 6.0, ((0, 8), (1, 16)))
    prompt_values = scatter_about(splits[4], (N_DP, PROMPT, KW), 1.0, 6.0, ((0, 8), (1, 16)))
    d_out = scatter_about(splits[5], (NB, BLOCK, QW), 1.0, 6.0, ((0, 128),))
    lengths = touch_ends(jax.random.randint(splits[6], (NB,), BLOCK // 8, BLOCK + 1), jax.random.fold_in(splits[6], 1), BLOCK // 8, BLOCK).astype(jnp.int32)
    owner = touch_ends(jax.random.randint(splits[7], (NB,), 0, N_DP), jax.random.fold_in(splits[7], 1), 0, N_DP - 1).astype(jnp.int32)
    return dict(queries=queries, resp_keys=resp_keys, resp_values=resp_values, prompt_keys=prompt_keys, prompt_values=prompt_values, d_out=d_out, lengths=lengths, owner=owner)


def attend(q_rows, d_rows, offset, stride, length, keys, values):
    rows = q_rows.shape[0]
    span = keys.shape[0]
    kv_heads = keys.shape[1] // HEAD_DIM
    group = q_rows.shape[1] // keys.shape[1]
    key_heads = keys.astype(jnp.float32).reshape(span, kv_heads, HEAD_DIM)
    val_heads = values.astype(jnp.float32).reshape(span, kv_heads, HEAD_DIM)
    key_pos = jnp.arange(span, dtype=jnp.int32) - (span - BLOCK)
    live_rows = jnp.clip((length - offset + stride - 1) // stride, 0, rows)
    turns = ((live_rows + TILE - 1) // TILE).astype(jnp.int32)
    scale = HEAD_DIM ** -0.5

    def step(turn, carry):
        out_all, dq_all, dk_sum, dv_sum = carry
        start = (turn * TILE).astype(jnp.int32)
        qt = lax.dynamic_slice_in_dim(q_rows, start, TILE, 0).astype(jnp.float32)
        qt = qt.reshape(TILE, kv_heads, group, HEAD_DIM)
        dt = lax.dynamic_slice_in_dim(d_rows, start, TILE, 0)
        pos = offset + stride * (start + jnp.arange(TILE, dtype=jnp.int32))
        live = pos < length
        dt = jnp.where(live[:, None], dt, jnp.zeros_like(dt))
        dt = dt.astype(jnp.float32).reshape(TILE, kv_heads, group, HEAD_DIM)
        scores = jnp.einsum("tkgd,skd->kgts", qt, key_heads) * scale
        allowed = key_pos[None, :] <= pos[:, None]
        scores = jnp.where(allowed, scores, -1e30)
        top = jnp.max(scores, axis=-1, keepdims=True)
        expd = jnp.exp(scores - top)
        probs = expd / jnp.sum(expd, axis=-1, keepdims=True)
        weights = lax.optimization_barrier(probs.astype(jnp.bfloat16)).astype(jnp.float32)
        out = jnp.einsum("kgts,skd->tkgd", weights, val_heads)
        out = out * live.astype(jnp.float32)[:, None, None, None]
        dprob = jnp.einsum("tkgd,skd->kgts", dt, val_heads)
        delta = jnp.einsum("tkgd,tkgd->kgt", dt, out)
        dscore = probs * (dprob - delta[..., None]) * scale
        dscore = lax.optimization_barrier(dscore.astype(jnp.bfloat16)).astype(jnp.float32)
        dq = jnp.einsum("kgts,skd->tkgd", dscore, key_heads)
        dk_sum = dk_sum + jnp.einsum("kgts,tkgd->skd", dscore, qt)
        dv_sum = dv_sum + jnp.einsum("kgts,tkgd->skd", weights, dt)
        out_all = lax.dynamic_update_slice_in_dim(out_all, out.reshape(TILE, -1).astype(jnp.bfloat16), start, 0)
        dq_all = lax.dynamic_update_slice_in_dim(dq_all, dq.reshape(TILE, -1).astype(jnp.bfloat16), start, 0)
        return out_all, dq_all, dk_sum, dv_sum

    init = (jnp.zeros((rows, q_rows.shape[1]), jnp.bfloat16),
            jnp.zeros((rows, q_rows.shape[1]), jnp.bfloat16),
            jnp.zeros((span, kv_heads, HEAD_DIM), jnp.float32),
            jnp.zeros((span, kv_heads, HEAD_DIM), jnp.float32))
    out_all, dq_all, dk_sum, dv_sum = lax.fori_loop(jnp.int32(0), turns, step, init)
    return out_all, dq_all, dk_sum.reshape(span, -1), dv_sum.reshape(span, -1)


def reference(queries, resp_keys, resp_values, prompt_keys, prompt_values, d_out, lengths, owner):
    groups = prompt_keys.shape[0]
    prompt_n = prompt_keys.shape[1]
    width_k = prompt_keys.shape[2]

    def one(accum, index):
        own = owner[index]
        pkeys = lax.dynamic_index_in_dim(prompt_keys, own, 0, keepdims=False)
        pvals = lax.dynamic_index_in_dim(prompt_values, own, 0, keepdims=False)
        keys = jnp.concatenate([pkeys, resp_keys[index]], axis=0)
        values = jnp.concatenate([pvals, resp_values[index]], axis=0)
        out, dq, dk, dv = attend(queries[index], d_out[index], 0, 1, lengths[index], keys, values)
        select = (jnp.arange(groups, dtype=jnp.int32) == own).astype(jnp.float32)
        term = jnp.concatenate([dk[:prompt_n], dv[:prompt_n]], axis=1)
        accum = accum + select[:, None, None] * term[None]
        return accum, (out, dq, dk[prompt_n:].astype(jnp.bfloat16), dv[prompt_n:].astype(jnp.bfloat16))

    start = jnp.zeros((groups, prompt_n, 2 * width_k), jnp.float32)
    accum, results = lax.scan(one, start, jnp.arange(queries.shape[0], dtype=jnp.int32))
    return results[0], results[1], results[2], results[3], accum[..., :width_k], accum[..., width_k:]
```

```python
import functools

import jax
import jax.numpy as jnp
from jax import lax
from jax.experimental import pallas as pl
from jax.experimental.pallas import tpu as pltpu
from jax.sharding import PartitionSpec as P

HEAD_DIM = 128
ROWS = 256
F32 = jnp.float32
BF16 = jnp.bfloat16
LOG2_E = 1.4426950408889634
ROW_BY_ROW = (((1,), (1,)), ((), ()))


def here_of():
    return lax.axis_index("dp") * lax.axis_size("rollout") + lax.axis_index("rollout")


def select_kernel(owner_ref, groups_ref, out_ref):
    base = lax.axis_index("dp") * lax.axis_size("rollout")
    for r in range(out_ref.shape[0]):
        out_ref[r] = groups_ref[owner_ref[base + r]]


def select_slices(owner, groups, count):
    return pl.pallas_call(
        select_kernel,
        out_shape=jax.ShapeDtypeStruct((count,) + groups.shape[1:], groups.dtype),
        in_specs=[pl.BlockSpec(memory_space=pltpu.SMEM), pl.BlockSpec(memory_space=pltpu.VMEM)],
        out_specs=pl.BlockSpec(memory_space=pltpu.VMEM),
        name="select_slices",
    )(owner, groups)


def group_sum_kernel(owner_ref, received_ref, out_ref, total):
    base = lax.axis_index("dp") * lax.axis_size("rollout")
    total[...] = jnp.zeros_like(total)
    for r in range(received_ref.shape[0]):
        total[owner_ref[base + r]] += received_ref[r].astype(F32)
    out_ref[...] = total[...].astype(out_ref.dtype)


def group_sums(owner, received, groups):
    shape = (groups,) + received.shape[1:]
    return pl.pallas_call(
        group_sum_kernel,
        out_shape=jax.ShapeDtypeStruct(shape, BF16),
        in_specs=[pl.BlockSpec(memory_space=pltpu.SMEM), pl.BlockSpec(memory_space=pltpu.VMEM)],
        out_specs=pl.BlockSpec(memory_space=pltpu.VMEM),
        scratch_shapes=[pltpu.VMEM(shape, F32)],
        name="group_sums",
    )(owner, received)


def final_sum_kernel(parts_ref, keys_ref, values_ref):
    total = parts_ref[0].astype(F32)
    for r in range(1, parts_ref.shape[0]):
        total += parts_ref[r].astype(F32)
    keys_ref[0] = total[0]
    values_ref[0] = total[1]


def final_sums(parts):
    out = jax.ShapeDtypeStruct((1,) + parts.shape[2:], F32)
    return pl.pallas_call(
        final_sum_kernel,
        out_shape=(out, out),
        in_specs=[pl.BlockSpec(memory_space=pltpu.VMEM)],
        out_specs=[pl.BlockSpec(memory_space=pltpu.VMEM)] * 2,
        name="final_sums",
    )(parts)


def attend_kernel(
    lengths_ref, q_ref, g_ref, resp_k_ref, resp_v_ref, prompt_k_ref, prompt_v_ref,
    out_ref, dq_ref, d_resp_k_ref, d_resp_v_ref, d_prompt_ref,
    keys, values, keys_t, values_t, dk_sum, dv_sum, *, group,
):
    length = lengths_ref[here_of()]
    scale = HEAD_DIM ** (-0.5)
    block = q_ref.shape[1]
    slices = prompt_k_ref.shape[0]
    prompt_n = keys.shape[0] - block
    keys[:prompt_n] = prompt_k_ref[:, 0].reshape(prompt_n, HEAD_DIM)
    keys[prompt_n:] = resp_k_ref[0]
    values[:prompt_n] = prompt_v_ref[:, 0].reshape(prompt_n, HEAD_DIM)
    values[prompt_n:] = resp_v_ref[0]
    keys_t[...] = keys[...].T
    values_t[...] = values[...].T
    dk_sum[...] = jnp.zeros_like(dk_sum)
    dv_sum[...] = jnp.zeros_like(dv_sum)

    def tile(t):
        span = prompt_n + (t + 1) * ROWS
        old = span - ROWS
        rows = pl.ds(t * ROWS, ROWS)
        live = (lax.broadcasted_iota(jnp.int32, (ROWS, HEAD_DIM), 0) + t * ROWS < length).astype(F32)
        allowed = lax.broadcasted_iota(jnp.int32, (ROWS, ROWS), 0) <= lax.broadcasted_iota(
            jnp.int32, (ROWS, ROWS), 1
        )
        for h in range(group):
            cols = pl.ds(h * HEAD_DIM, HEAD_DIM)
            q = q_ref[0, rows, cols]
            g_wide = g_ref[0, rows, cols].astype(F32) * live
            g = g_wide.astype(BF16)
            scores = lax.dot_general(keys[:span], q, ROW_BY_ROW, preferred_element_type=F32)
            dprobs = lax.dot_general(values[:span], g, ROW_BY_ROW, preferred_element_type=F32)
            scores = jnp.concatenate([scores[:old], jnp.where(allowed, scores[old:], -1e30)], axis=0)
            top = jnp.max(scores, axis=0, keepdims=True)
            probs = jnp.exp2((scores - top) * (scale * LOG2_E))
            probs = probs * (1.0 / jnp.sum(probs, axis=0, keepdims=True))
            weights = probs.astype(BF16)
            out_t = jnp.dot(values_t[:, :span], weights, preferred_element_type=F32)
            delta = jnp.sum(g_wide.T * out_t, axis=0, keepdims=True)
            dscores = (probs * (dprobs - delta) * scale).astype(BF16)
            dq_t = jnp.dot(keys_t[:, :span], dscores, preferred_element_type=F32)
            dk_sum[:span] += jnp.dot(dscores, q, preferred_element_type=F32)
            dv_sum[:span] += jnp.dot(weights, g, preferred_element_type=F32)
            out_ref[0, rows, cols] = (out_t.T * live).astype(BF16)
            dq_ref[0, rows, cols] = dq_t.T.astype(BF16)

    for t in range(block // ROWS):

        @pl.when(length > t * ROWS)
        def _():
            tile(t)

        @pl.when(length <= t * ROWS)
        def _():
            dead = jnp.zeros((ROWS, out_ref.shape[2]), BF16)
            out_ref[0, pl.ds(t * ROWS, ROWS)] = dead
            dq_ref[0, pl.ds(t * ROWS, ROWS)] = dead

    d_resp_k_ref[0] = dk_sum[prompt_n:].astype(BF16)
    d_resp_v_ref[0] = dv_sum[prompt_n:].astype(BF16)
    d_prompt_ref[:, 0] = dk_sum[:prompt_n].astype(BF16).reshape(slices, prompt_n // slices, HEAD_DIM)
    d_prompt_ref[:, 1] = dv_sum[:prompt_n].astype(BF16).reshape(slices, prompt_n // slices, HEAD_DIM)


def attend(lengths, q, g, resp_k, resp_v, prompt):
    block = q.shape[1]
    kv_heads = resp_k.shape[2] // HEAD_DIM
    group = q.shape[2] // resp_k.shape[2]
    slices, _, slice_rows, _ = prompt.shape
    span = slices * slice_rows + block
    wide = pl.BlockSpec((1, block, group * HEAD_DIM), lambda e, n: (0, 0, e))
    narrow = pl.BlockSpec((1, block, HEAD_DIM), lambda e, n: (0, 0, e))
    prompt_keys = pl.BlockSpec((slices, 1, slice_rows, HEAD_DIM), lambda e, n: (0, 0, 0, e))
    prompt_values = pl.BlockSpec((slices, 1, slice_rows, HEAD_DIM), lambda e, n: (0, 1, 0, e))
    both = pl.BlockSpec((slices, 2, slice_rows, HEAD_DIM), lambda e, n: (0, 0, 0, e))
    like = lambda x: jax.ShapeDtypeStruct(x.shape, BF16)
    return pl.pallas_call(
        functools.partial(attend_kernel, group=group),
        out_shape=(like(q), like(q), like(resp_k), like(resp_k), like(prompt)),
        grid_spec=pltpu.PrefetchScalarGridSpec(
            num_scalar_prefetch=1,
            grid=(kv_heads,),
            in_specs=[wide, wide, narrow, narrow, prompt_keys, prompt_values],
            out_specs=[wide, wide, narrow, narrow, both],
            scratch_shapes=[pltpu.VMEM((span, HEAD_DIM), BF16)] * 2
            + [pltpu.VMEM((HEAD_DIM, span), BF16)] * 2
            + [pltpu.VMEM((span, HEAD_DIM), F32)] * 2,
        ),
        compiler_params=pltpu.CompilerParams(vmem_limit_bytes=56 << 20),
        name="attend",
    )(lengths, q, g, resp_k, resp_v, prompt, prompt)


def exchange(pieces, axis):
    return lax.all_to_all(pieces, axis, split_axis=0, concat_axis=0, tiled=True)


def per_device(queries, resp_keys, resp_values, prompt_keys, prompt_values, d_out, lengths, owner):
    rollout_count = lax.axis_size("rollout")
    groups = lax.axis_size("dp")
    local = jnp.concatenate([prompt_keys, prompt_values], axis=0)
    every_group = exchange(jnp.broadcast_to(local[None], (groups,) + local.shape), "dp")
    prompt = exchange(select_slices(owner, every_group, rollout_count), "rollout")
    out, dq, dk, dv, d_prompt = attend(lengths, queries, d_out, resp_keys, resp_values, prompt)
    received = exchange(d_prompt, "rollout")
    parts = exchange(group_sums(owner, received, groups), "dp")
    d_prompt_keys, d_prompt_values = final_sums(parts)
    return out, dq, dk, dv, d_prompt_keys, d_prompt_values


def solution(mesh):
    by_block = P(("dp", "rollout"), None, None)
    by_prompt = P("dp", "rollout", None)
    return jax.shard_map(
        per_device,
        mesh=mesh,
        in_specs=(by_block, by_block, by_block, by_prompt, by_prompt, by_block, P(), P()),
        out_specs=(by_block, by_block, by_block, by_block, by_prompt, by_prompt),
        check_vma=False,
    )
```
